32 devices in a mesh: rep: 1, r: 8 (over y, z), s: 4 (over x, core).
Axes of the slice: x: 2, y: 2, z: 4, core: 2. Of those that a mesh axis runs over, the one named last changes fastest.
Arguments:
- x: bfloat16 [32, 4096, 512], P(('rep', 'r', 's'))
- dy: bfloat16 [32, 4096, 512], P(('rep', 'r', 's'))
- w_gate: bfloat16 [2, 512, 1280], P(None, 's')
- w_up: bfloat16 [2, 512, 1280], P(None, 's')
- w_down: bfloat16 [2, 1280, 512], P(None, 's')
Outputs:
- output 1: bfloat16 [32, 4096, 512], P(('rep', 'r', 's'))
- output 2: bfloat16 [2, 512, 1280], P('rep', 's')
- output 3: bfloat16 [2, 512, 1280], P('rep', 's')
- output 4: bfloat16 [2, 1280, 512], P('rep', 's')
All inputs are finite; a program needn't handle non-finite values.
Results may differ from the reference program's by a relative error of at most 0.018.
Values are sent between devices in bfloat16 or wider.
A program may use at most 2 GiB of HBM per device.

```python
import jax
import jax.numpy as jnp
from jax import lax

SEQUENCES = 32
TOKENS = 4096
D = 512
FF = 1280
LAYERS = 2
NAMES = ("w_gate", "w_up", "w_down")
SHAPES = {"w_gate": (LAYERS, D, FF), "w_up": (LAYERS, D, FF), "w_down": (LAYERS, FF, D)}


def bump(key, n, height):
    away = (jnp.arange(n, dtype=jnp.int32) - jax.random.randint(key, (), 0, n, jnp.int32)) % n
    return jnp.where(away < n // 8, height, 1.0)


def together(key, own, strength):
    shared = jax.random.normal(key, own.shape[1:], jnp.float32)
    return (own + strength * shared) * lax.rsqrt(1 + strength * strength)


def setup_inputs(seed: int = 0, part: int = 0) -> dict:
    kx, kdy, ka, kb, kz, kf, kh, kl, *kw = jax.random.split(jax.random.key(seed), 8 + len(NAMES))
    kx, kdy, ka, kb = (jax.random.fold_in(k, part) for k in (kx, kdy, ka, kb))
    shape = (SEQUENCES, TOKENS, D)
    much_x, much_dy = jax.random.uniform(kz, (2,), jnp.float32, 0.0, 1.0)
    layers = 2.0 ** jax.random.uniform(kl, (LAYERS, 1, 1), jnp.float32, -1.0, 1.0)
    x = together(ka, jax.random.normal(kx, shape, jnp.float32), much_x) * bump(kf, D, 4.0)
    dy = together(kb, jax.random.normal(kdy, shape, jnp.float32), much_dy)
    drawn = {"x": x.astype(jnp.bfloat16), "dy": (dy * (SEQUENCES * TOKENS) ** -0.5).astype(jnp.bfloat16)}
    for key, name in zip(kw, NAMES, strict=True):
        w = jax.random.normal(key, SHAPES[name], jnp.float32) * SHAPES[name][1] ** -0.5
        drawn[name] = (w * {"w_gate": 1.0, "w_up": bump(kh, FF, 4.0), "w_down": layers}[name]).astype(jnp.bfloat16)
    return drawn


def matmul(a, w):
    return jnp.dot(a, w, preferred_element_type=jnp.float32).astype(jnp.bfloat16)


def normed(h):
    wide = h.astype(jnp.float32)
    scale = lax.rsqrt(jnp.mean(wide**2, -1, keepdims=True) + 1e-6)
    return (wide * scale).astype(jnp.bfloat16)


def layer(h, w):
    a = normed(h)
    gate = jnp.dot(a, w["w_gate"], preferred_element_type=jnp.float32)
    up = jnp.dot(a, w["w_up"], preferred_element_type=jnp.float32)
    return h + matmul((jax.nn.silu(gate) * up).astype(jnp.bfloat16), w["w_down"])


def stack(weights, h):
    return lax.scan(lambda h, w: (layer(h, w), None), h, weights)[0]


def reference(x, dy, w_gate, w_up, w_down):
    weights = dict(zip(NAMES, (w_gate, w_up, w_down), strict=True))

    def take(so_far, sequence):
        h, by_y = sequence
        _, back = jax.vjp(stack, weights, h)
        by_weights, by_h = back(by_y)
        return jax.tree.map(lambda total, term: total + term.astype(jnp.float32), so_far, by_weights), by_h

    none_yet = {name: jnp.zeros(w.shape, jnp.float32) for name, w in weights.items()}
    by_weights, by_x = lax.scan(take, none_yet, (x, dy))
    return (by_x, *(by_weights[name].astype(jnp.bfloat16) for name in NAMES))
```

```python
import functools

import jax
import jax.numpy as jnp
from jax import lax
from jax.experimental import pallas as pl
from jax.experimental.pallas import tpu as pltpu
from jax.sharding import PartitionSpec as P

MESH = pl.DeviceIdType.MESH
BF, F32 = jnp.bfloat16, jnp.float32
LAYERS, D, FF = 2, 512, 1280
HALF = FF // 2
CHUNKS = HALF // 128
STEPS = LAYERS * CHUNKS


def nn(a, b):
    return jnp.dot(a, b, preferred_element_type=F32)


def nt(a, b):
    return lax.dot_general(a, b, (((1,), (1,)), ((), ())), preferred_element_type=F32)


def tn(a, b):
    return lax.dot_general(a, b, (((0,), (0,)), ((), ())), preferred_element_type=F32)


def scale_of(wide):
    return lax.rsqrt(jnp.mean(wide * wide, -1, keepdims=True) + 1e-6)


def gated(gate):
    sig = 0.5 * jnp.tanh(0.5 * gate) + 0.5
    return sig, gate * sig


def kernel(
    x_ref, dy_ref, wg_ref, wu_ref, wd_ref,
    dx_ref, og_ref, ou_ref, od_ref,
    WG, WU, WD, XH, A, G, DA, ACT, ACC, ACD, DGU, AC2, WC, WDC,
    S0, s0s, s0r, S1, s1s, s1r, S2, s2s, s2r, S3, s3s, s3r, fin, dnx,
    lsem, xsem, gss, grs, ss, rs, zs, zr, ags, agr, dns, dnr,
):
    r, s = lax.axis_index("r"), lax.axis_index("s")
    y, z = r // 4, r % 4
    xx, core = s // 2, s % 2
    tokens = XH.shape[0]
    tt = tokens // 4
    partner = {"s": 2 * xx + (1 - core)}
    xn = {"s": 2 * (1 - xx) + core}

    def place(dy_, dz_):
        return {"r": ((y + dy_) % 2) * 4 + (z + dz_) % 4}

    others = [(a, b) for a in range(2) for b in range(4) if (a, b) != (0, 0)]

    barrier = pltpu.get_barrier_semaphore()
    for dev in [partner, xn] + [place(*o) for o in others]:
        pl.semaphore_signal(barrier, inc=1, device_id=dev, device_id_type=MESH)
    pl.semaphore_wait(barrier, 2 + len(others))

    def remote(src, dst, send, recv, dev):
        return pltpu.make_async_remote_copy(src_ref=src, dst_ref=dst, send_sem=send, recv_sem=recv, device_id=dev, device_id_type=MESH)

    mats = [(wg_ref, WG, D // 4), (wu_ref, WU, D // 4), (wd_ref, WD, FF // 4)]
    far = 2 * (1 - xx) + core

    def rows(W, layer, start, n):
        return W.at[layer, pl.ds(pl.multiple_of(start, 32), n), :]

    def fetch(layer, m, kind):
        shard, W, n = mats[m]
        i, h = 3 * layer + m, n // 2
        if kind == "own":
            return pltpu.make_async_copy(shard.at[layer], rows(W, layer, n * s, n), lsem.at[i])
        if kind == "near":
            src, dst, row, dev = shard.at[layer], rows(W, layer, n * s, n), 0, partner
        elif kind == "across":
            src, dst, row, dev = shard.at[layer, pl.ds(pl.multiple_of(h * y, 32), h), :], rows(W, layer, n * s + h * y, h), 1, xn
        else:
            start = n * far + h * (1 - y if kind == "other_near" else y)
            src = dst = rows(W, layer, start, h)
            row, dev = {"to_y": (2, place(1, 0)), "mine_near": (3, partner), "other_near": (4, partner)}[kind]
        return remote(src, dst, gss.at[row, i], grs.at[row, i], dev)

    def begin(layer, m):
        for kind in ("across", "near", "own"):
            fetch(layer, m, kind).start()

    def pass_x(layer, m):
        fetch(layer, m, "across").wait_recv()
        fetch(layer, m, "to_y").start()
        fetch(layer, m, "mine_near").start()

    def pass_y(layer, m):
        fetch(layer, m, "to_y").wait_recv()
        fetch(layer, m, "other_near").start()

    def arrived(layer, m):
        fetch(layer, m, "own").wait()
        for kind in ("near", "mine_near", "other_near"):
            fetch(layer, m, kind).wait_recv()

    for m in range(3):
        begin(0, m)
    tile = [pl.ds(t * tt, tt) for t in range(4)]
    load_x = [pltpu.make_async_copy(x_ref.at[t, :], XH.at[t, :], xsem.at[i]) for i, t in enumerate(tile)]
    load_dy = pltpu.make_async_copy(dy_ref, G, xsem.at[4])
    for copy in load_x:
        copy.start()
    load_dy.start()
    for t in range(4):
        load_x[t].wait()
        wide = XH[tile[t], :].astype(F32)
        A[0, tile[t], :] = (wide * scale_of(wide)).astype(BF)
    for m in range(3):
        pass_x(0, m)
    for m in range(3):
        begin(1, m)
    for m in range(3):
        pass_y(0, m)
    arrived(0, 0)
    arrived(0, 1)

    def up_front(t):
        a = A[0, tile[t], :]
        for f in range(FF // 256):
            c = slice(256 * f, 256 * f + 256)
            gate, up = nn(a, WG[0, :, c]), nn(a, WU[0, :, c])
            ACT[t % 2, :, c] = (gated(gate)[1] * up).astype(BF)

    def down_back(t):
        out = nn(ACT[t % 2], WD[0]).astype(BF).astype(F32)
        h = (XH[tile[t], :].astype(F32) + out).astype(BF)
        XH[tile[t], :] = h
        wide = h.astype(F32)
        A[1, tile[t], :] = (wide * scale_of(wide)).astype(BF)

    up_front(0)
    arrived(0, 2)
    for t in range(3):
        up_front(t + 1)
        down_back(t)
        if t == 0:
            pass_x(1, 0)
            pass_x(1, 1)
        if t == 1:
            pass_x(1, 2)
            pass_y(1, 0)
            pass_y(1, 1)
        if t == 2:
            pass_y(1, 2)
    down_back(3)
    for m in range(3):
        arrived(1, m)
    for layer in range(2):
        for m in range(3):
            for kind in ("near", "across", "to_y", "mine_near", "other_near"):
                fetch(layer, m, kind).wait_send()
    load_dy.wait()

    def pair(k, j, dev, src, dst):
        return remote(src, dst, ss.at[j, k % 2], rs.at[j, k % 2], dev)

    def core_copy(k):
        return pair(k, 0, partner, s0s, s0r.at[k % 2])

    def x_copy(k):
        return pair(k, 1, xn, s1s, s1r.at[k % 2])

    def y_copy(k):
        return pair(k, 2, place(1, 0), s2s, s2r.at[k % 2])

    def lanes(n):
        return pl.ds(pl.multiple_of(128 * n, 128), 128)

    def z_copies(k):
        return [
            remote(s3s.at[:, lanes((z + j) % 4)], s3r.at[k % 2, j - 1], zs.at[k % 2, j - 1], zr.at[k % 2, j - 1], place(0, j)) for j in range(1, 4)
        ]

    def piece(k):
        return fin.at[k, pl.ds(pl.multiple_of(96 * y, 32), 96), lanes(z)]

    def all_copies(k):
        return [remote(piece(k), piece(k), ags.at[k, i], agr.at[k, i], place(*o)) for i, o in enumerate(others)]

    def send_core():
        for x_ in range(2):
            for q in range(2):
                for buf, who in ((s0s, 1 - core), (S0, core)):
                    gu = ACC[pl.ds(pl.multiple_of(256 * x_ + 128 * who + 64 * q, 64), 64), :]
                    dn = ACD[pl.ds(pl.multiple_of(128 * x_ + 64 * who + 32 * q, 32), 32), :]
                    buf[x_, 96 * q : 96 * q + 64, :] = gu.astype(buf.dtype)
                    buf[x_, 96 * q + 64 : 96 * q + 96, :] = dn.astype(buf.dtype)

    def after_core(k):
        core_copy(k).wait()
        s1s[...] = (S0[1 - xx] + s0r[k % 2, 1 - xx].astype(F32)).astype(BF)
        x_copy(k).start()
        S1[...] = S0[xx] + s0r[k % 2, xx].astype(F32)

    def after_x(k):
        x_copy(k).wait()
        give, keep = (pl.ds(pl.multiple_of(96 * h, 32), 96) for h in (1 - y, y))
        s2s[...] = (S1[give, :] + s1r[k % 2, give, :].astype(F32)).astype(BF)
        y_copy(k).start()
        S2[...] = S1[keep, :] + s1r[k % 2, keep, :].astype(F32)

    def after_y(k):
        y_copy(k).wait()
        S3[...] = S2[...] + s2r[k % 2].astype(F32)
        s3s[...] = S3[...].astype(BF)
        for copy in z_copies(k):
            copy.start()

    def after_z(k):
        for copy in z_copies(k):
            copy.wait()
        total = S3[:, lanes(z)]
        for j in range(3):
            total += s3r[k % 2, j].astype(F32)
        piece(k)[...] = total.astype(BF)
        for copy in all_copies(k):
            copy.start()

    def after_all(k):
        for copy in all_copies(k):
            copy.wait()

    def when(cond, f, k):
        pl.when(cond)(lambda: f(k))

    def at(t):
        return pl.ds(pl.multiple_of(t * tt, tt), tt)

    def into(t, layer):
        wide, by_a = XH[at(t), :].astype(F32), DA[at(t), :].astype(BF).astype(F32)
        scale = scale_of(wide)
        back = by_a * scale - wide * (scale * scale * scale * jnp.mean(by_a * wide, -1, keepdims=True))
        G[at(t), :] = (G[at(t), :].astype(F32) + back.astype(BF).astype(F32)).astype(BF)

    def step(k, carry):
        layer, c = 1 - k // CHUNKS, k % CHUNKS

        @pl.when(k == CHUNKS)
        def _():
            def one(t, carry):
                into(t, 1)
                return carry

            lax.fori_loop(0, 4, one, 0)
            for copy in load_x:
                copy.start()

        @pl.when(c == 0)
        def _():
            DA[...] = jnp.zeros_like(DA)

        lo, hi = lanes(c), lanes(c + CHUNKS)
        WC[:, 0:128], WC[:, 128:256] = WG[layer, :, lo], WG[layer, :, hi]
        WC[:, 256:384], WC[:, 384:512] = WU[layer, :, lo], WU[layer, :, hi]
        WDC[0:128, :], WDC[128:256, :] = WD[layer, lo, :], WD[layer, hi, :]
        ACC[...] = jnp.zeros_like(ACC)
        ACD[...] = jnp.zeros_like(ACD)

        def front(t):
            gu = nn(A[layer, tile[t], :], WC[...])
            gate, up = gu[:, 0:256], gu[:, 256:512]
            by_act = nt(G[tile[t], :], WDC[...]).astype(BF).astype(F32)
            sig, silu = gated(gate)
            AC2[t % 2] = (silu * up).astype(BF)
            DGU[t % 2, :, 0:256] = (by_act * up * (sig * (1.0 + (gate - silu)))).astype(BF)
            DGU[t % 2, :, 256:512] = (by_act * silu).astype(BF)

        def back(t):
            ACC[...] += tn(A[layer, tile[t], :], DGU[t % 2])
            ACD[...] += tn(AC2[t % 2], G[tile[t], :])
            DA[tile[t], :] += nt(DGU[t % 2], WC[...])

        front(0)
        front(1)
        back(0)
        when(k >= 1, after_core, k - 1)
        front(2)
        back(1)
        when(k >= 2, after_y, k - 2)
        when(k >= 3, after_all, k - 3)
        front(3)
        back(2)
        back(3)
        when(k >= 2, after_z, k - 2)
        when(k >= 1, after_x, k - 1)
        send_core()
        core_copy(k).start()
        return carry

    lax.fori_loop(0, STEPS, step, 0)

    last = STEPS - 1
    after_core(last)
    after_y(last - 1)
    for copy in load_x:
        copy.wait()
    store_dx = [pltpu.make_async_copy(G.at[t, :], dx_ref.at[t, :], xsem.at[i]) for i, t in enumerate(tile)]
    for t in range(2):
        into(t, 0)
        store_dx[t].start()
    after_z(last - 1)
    after_x(last)
    for t in range(2, 4):
        into(t, 0)
        store_dx[t].start()
    after_y(last)
    after_all(last - 2)
    after_all(last - 1)

    def down_copies(layer):
        first = (1 - layer) * CHUNKS + (CHUNKS - 2) * (1 - core)
        return [
            remote(fin.at[pl.ds(first, 2), 96 * q + 64 : 96 * q + 96, :], dnx.at[layer, :, 32 * q : 32 * q + 32, :], dns.at[layer, q], dnr.at[layer, q], partner)
            for q in range(2)
        ]

    def put_out(layer):
        base = (1 - layer) * CHUNKS
        for c in range(CHUNKS):
            for q in range(2):
                block = fin[base + c, 96 * q : 96 * q + 64, :]
                rows_ = slice(64 * q, 64 * q + 64)
                for n, (out, start) in enumerate(((og_ref, 0), (og_ref, HALF), (ou_ref, 0), (ou_ref, HALF))):
                    out[layer, rows_, start + 128 * c : start + 128 * c + 128] = block[:, 128 * n : 128 * n + 128]
        for n in range(3):
            for q in range(2):
                od_ref[layer, 128 * n + 32 * q : 128 * n + 32 * q + 32, :] = fin[base + n + 2 * core, 96 * q + 64 : 96 * q + 96, :]
        for n in range(2):
            od_ref[layer, 128 * n + 64 : 128 * n + 128, :] = dnx[layer, n]

    for copy in down_copies(1):
        copy.start()
    after_z(last)
    for copy in down_copies(1):
        copy.wait()
    put_out(1)
    after_all(last)
    for copy in down_copies(0):
        copy.start()
    for copy in down_copies(0):
        copy.wait()
    put_out(0)
    for copy in store_dx:
        copy.wait()


def solution(mesh):
    def step(x, dy, wg, wu, wd):
        tokens = x.shape[1]
        tt = tokens // 4
        hbm, vmem = pl.BlockSpec(memory_space=pl.ANY), pl.BlockSpec(memory_space=pltpu.VMEM)
        V, DMA = pltpu.VMEM, pltpu.SemaphoreType.DMA
        dx, *grads = pl.pallas_call(
            kernel,
            out_shape=[
                jax.ShapeDtypeStruct((tokens, D), BF),
                *(jax.ShapeDtypeStruct(w.shape, BF) for w in (wg, wu, wd)),
            ],
            in_specs=[hbm] * 5,
            out_specs=[hbm, vmem, vmem, vmem],
            scratch_shapes=[
                V((LAYERS, D, FF), BF), V((LAYERS, D, FF), BF), V((LAYERS, FF, D), BF),
                V((tokens, D), BF), V((LAYERS, tokens, D), BF), V((tokens, D), BF), V((tokens, D), F32),
                V((2, tt, FF), BF), V((D, 512), F32), V((256, D), F32), V((2, tt, 512), BF), V((2, tt, 256), BF),
                V((D, 512), BF), V((256, D), BF),
                V((2, 192, 512), F32), V((2, 192, 512), BF), V((2, 2, 192, 512), BF),
                V((192, 512), F32), V((192, 512), BF), V((2, 192, 512), BF),
                V((96, 512), F32), V((96, 512), BF), V((2, 96, 512), BF),
                V((96, 512), F32), V((96, 512), BF), V((2, 3, 96, 128), BF),
                V((STEPS, 192, 512), BF), V((LAYERS, 2, 64, 512), BF),
                DMA((6,)), DMA((5,)), DMA((5, 6)), DMA((5, 6)), DMA((3, 2)), DMA((3, 2)),
                DMA((2, 3)), DMA((2, 3)), DMA((STEPS, 7)), DMA((STEPS, 7)), DMA((2, 2)), DMA((2, 2)),
            ],
            compiler_params=pltpu.CompilerParams(collective_id=0, has_side_effects=True, vmem_limit_bytes=67_043_328),
        )(x[0], dy[0], wg, wu, wd)
        return (dx[None], *grads)

    states, cut = P(("rep", "r", "s"), None, None), P(None, "s", None)
    return jax.shard_map(
        step,
        mesh=mesh,
        in_specs=(states, states) + (cut,) * 3,
        out_specs=(states,) + (P("rep", "s", None),) * 3,
        check_vma=False,
    )
```

```python
import functools

import jax
import jax.numpy as jnp
from jax import lax
from jax.experimental import pallas as pl
from jax.experimental.pallas import tpu as pltpu
from jax.sharding import PartitionSpec as P

MESH = pl.DeviceIdType.MESH
BF, F32 = jnp.bfloat16, jnp.float32
LAYERS, D, FF = 2, 512, 1280
HALF = FF // 2
CHUNKS = HALF // 128
STEPS = LAYERS * CHUNKS


def nn(a, b):
    return jnp.dot(a, b, preferred_element_type=F32)


def nt(a, b):
    return lax.dot_general(a, b, (((1,), (1,)), ((), ())), preferred_element_type=F32)


def tn(a, b):
    return lax.dot_general(a, b, (((0,), (0,)), ((), ())), preferred_element_type=F32)


def scale_of(wide):
    return lax.rsqrt(jnp.mean(wide * wide, -1, keepdims=True) + 1e-6)


def gated(gate):
    sig = 0.5 * jnp.tanh(0.5 * gate) + 0.5
    return sig, gate * sig


def kernel(
    x_ref, dy_ref, wg_ref, wu_ref, wd_ref,
    dx_ref, og_ref, ou_ref, od_ref,
    W, WD, XH, A, G, DGU, ACC, ACD, AC2,
    S0, s0s, s0r, S1, s1s, s1r, S2, s2s, s2r, S3, s3s, s3r, fin, dnx,
    lsem, ldsem, xsem, asem, osem, gss, grs, ss, rs, zs, zr, azs, azr, ays, ayr, dns, dnr,
):
    r, s = lax.axis_index("r"), lax.axis_index("s")
    y, z = r // 4, r % 4
    xx, core = s // 2, s % 2
    tokens = XH.shape[0]
    tt = tokens // 4
    partner = {"s": 2 * xx + (1 - core)}
    xn = {"s": 2 * (1 - xx) + core}

    def place(dy_, dz_):
        return {"r": ((y + dy_) % 2) * 4 + (z + dz_) % 4}

    others = [(a, b) for a in range(2) for b in range(4) if (a, b) != (0, 0)]

    def lanes(n):
        return pl.ds(pl.multiple_of(128 * n, 128), 128)

    def some(start, n):
        return pl.ds(pl.multiple_of(start, 32), n)

    def remote(src, dst, send, recv, dev):
        return pltpu.make_async_remote_copy(src_ref=src, dst_ref=dst, send_sem=send, recv_sem=recv, device_id=dev, device_id_type=MESH)

    def local_gu(layer, c, n):
        shard, half = ((wg_ref, 0), (wg_ref, CHUNKS), (wu_ref, 0), (wu_ref, CHUNKS))[n]
        return pltpu.make_async_copy(shard.at[layer, :, lanes(c + half)], W.at[layer, c, some(128 * s, 128), 128 * n : 128 * n + 128], lsem.at[layer, c, n])

    def unit(who, layer, i):
        n = 5 * (who % 2) + i
        return 256 * (n // 2) + 128 * (who // 2) + 64 * (n % 2)

    def local_d(layer, i):
        return pltpu.make_async_copy(wd_ref.at[layer, 64 * i : 64 * i + 64, :], WD.at[layer, some(unit(s, layer, i), 64), :], ldsem.at[layer, i])

    tile = [pl.ds(t * tt, tt) for t in range(4)]
    load_x = [pltpu.make_async_copy(x_ref.at[t, :], XH.at[t, :], xsem.at[i]) for i, t in enumerate(tile)]
    load_dy = pltpu.make_async_copy(dy_ref, G, xsem.at[4])
    for c in range(CHUNKS):
        for n in range(4):
            local_gu(0, c, n).start()
    for copy in load_x:
        copy.start()
    for i in range(5):
        local_d(0, i).start()
    for c in range(CHUNKS):
        for n in range(4):
            local_gu(1, c, n).start()
    for i in range(5):
        local_d(1, i).start()
    load_dy.start()

    barrier = pltpu.get_barrier_semaphore()
    for dev in [partner, xn] + [place(*o) for o in others]:
        pl.semaphore_signal(barrier, inc=1, device_id=dev, device_id_type=MESH)
    pl.semaphore_wait(barrier, 2 + len(others))

    far = 2 * (1 - xx) + core
    KINDS = ("near", "across", "to_y", "mine_near", "other_near")

    def fetch(layer, p, kind):
        who = s if kind in ("near", "across") else far
        row = KINDS.index(kind)
        dev = (partner, xn, place(1, 0), partner, partner)[row]
        half = 1 - y if kind == "other_near" else y
        if isinstance(p, int) and p >= CHUNKS:
            start = unit(who, layer, p - CHUNKS)
            ref = WD.at[layer, some(start, 64) if kind == "near" else some(start + 32 * half, 32), :]
        else:
            ref = W.at[layer, p, some(128 * who, 128) if kind == "near" else some(128 * who + 64 * half, 64), :]
        return remote(ref, ref, gss.at[layer, row, p], grs.at[layer, row, p], dev)

    def begin(layer, p):
        if p >= CHUNKS:
            local_d(layer, p - CHUNKS).wait()
        else:
            for n in range(4):
                local_gu(layer, p, n).wait()
        fetch(layer, p, "across").start()
        fetch(layer, p, "near").start()

    def pass_x(layer, p):
        fetch(layer, p, "across").wait_recv()
        fetch(layer, p, "to_y").start()
        fetch(layer, p, "mine_near").start()

    def pass_y(layer, p):
        fetch(layer, p, "to_y").wait_recv()
        fetch(layer, p, "other_near").start()

    def arrived(layer, p):
        for kind in ("near", "mine_near", "other_near"):
            fetch(layer, p, kind).wait_recv()

    downs = range(CHUNKS, CHUNKS + 5)
    for p in range(CHUNKS + 5):
        begin(0, p)
    save_a = [pltpu.make_async_copy(A.at[t, :], dx_ref.at[t, :], asem.at[i]) for i, t in enumerate(tile)]
    for t in range(4):
        load_x[t].wait()
        wide = XH[tile[t], :].astype(F32)
        A[tile[t], :] = (wide * scale_of(wide)).astype(BF)
        save_a[t].start()

    pass_x(0, 0)
    pass_x(0, 1)
    pass_x(0, 2)
    pass_y(0, 0)

    def up_front(c, carry):
        @pl.when(c + 3 < CHUNKS)
        def _():
            pass_x(0, c + 3)

        @pl.when(c + 1 < CHUNKS)
        def _():
            pass_y(0, c + 1)

        @pl.when(c == 3)
        def _():
            for p in downs:
                pass_x(0, p)
            for p in downs:
                begin(1, p)

        @pl.when(c == 4)
        def _():
            for p in downs:
                pass_y(0, p)
            for p in range(CHUNKS):
                begin(1, p)

        arrived(0, c)
        for t in range(4):
            gu = nn(A[tile[t], :], W[0, c])
            gate, up = gu[:, 0:256], gu[:, 256:512]
            DGU[c // 2, tile[t], pl.ds(pl.multiple_of(256 * (c % 2), 256), 256)] = (gated(gate)[1] * up).astype(BF)
        return carry

    lax.fori_loop(0, CHUNKS, up_front, 0)
    for p in downs:
        arrived(0, p)
    for copy in save_a:
        copy.wait()

    def down_back(t):
        out = nn(DGU[0, tile[t], :], WD[0, 0:512, :]) + nn(DGU[1, tile[t], :], WD[0, 512:1024, :]) + nn(DGU[2, tile[t], 0:256], WD[0, 1024:1280, :])
        h = (XH[tile[t], :].astype(F32) + out.astype(BF).astype(F32)).astype(BF)
        XH[tile[t], :] = h
        wide = h.astype(F32)
        A[tile[t], :] = (wide * scale_of(wide)).astype(BF)

    down_back(0)
    down_back(1)
    down_back(2)
    for p in downs:
        pass_x(1, p)
    down_back(3)
    for p in range(3):
        pass_x(1, p)
    for p in downs:
        pass_y(1, p)
    pass_y(1, 0)
    for p in downs:
        arrived(1, p)
    load_dy.wait()

    def pair(k, j, dev, src, dst):
        return remote(src, dst, ss.at[j, k % 2], rs.at[j, k % 2], dev)

    def core_copy(k):
        return pair(k, 0, partner, s0s, s0r.at[k % 2])

    def x_copies(k):
        return [pair(k, 1 + i, xn, s1s.at[some(96 * h, 96), :], s1r.at[k % 2, some(96 * h, 96), :]) for i, h in enumerate((1 - y, y))]

    def y_copy(k):
        return pair(k, 3, place(1, 0), s2s, s2r.at[k % 2])

    def z_copies(k):
        return [
            remote(s3s.at[:, lanes((z + j) % 4)], s3r.at[k % 2, j - 1], zs.at[k % 2, j - 1], zr.at[k % 2, j - 1], place(0, j)) for j in range(1, 4)
        ]

    def piece(k, z_=z):
        return fin.at[k, some(96 * y, 96), lanes(z_)]

    def out_z(k):
        return [remote(piece(k), piece(k), azs.at[k % 4, j - 1], azr.at[k % 4, j - 1], place(0, j)) for j in range(1, 4)]

    def out_y(k):
        return [remote(piece(k, (z + j) % 4), piece(k, (z + j) % 4), ays.at[k % 4, j], ayr.at[k % 4, j], place(1, 0)) for j in range(4)]

    def send_core():
        for x_ in range(2):
            for q in range(2):
                for buf, who in ((s0s, 1 - core), (S0, core)):
                    gu = ACC[pl.ds(pl.multiple_of(256 * x_ + 128 * who + 64 * q, 64), 64), :]
                    dn = ACD[some(128 * x_ + 64 * who + 32 * q, 32), :]
                    buf[x_, 96 * q : 96 * q + 64, :] = gu.astype(buf.dtype)
                    buf[x_, 96 * q + 64 : 96 * q + 96, :] = dn.astype(buf.dtype)

    def after_core(k):
        core_copy(k).wait()
        for copy, h in zip(x_copies(k), (1 - y, y), strict=True):
            half = some(96 * h, 96)
            s1s[half, :] = (S0[1 - xx, half, :] + s0r[k % 2, 1 - xx, half, :].astype(F32)).astype(BF)
            copy.start()
        S1[...] = S0[xx] + s0r[k % 2, xx].astype(F32)

    def after_x(k):
        x_copies(k)[0].wait()
        give, keep = (some(96 * h, 96) for h in (1 - y, y))
        s2s[...] = (S1[give, :] + s1r[k % 2, give, :].astype(F32)).astype(BF)
        y_copy(k).start()
        x_copies(k)[1].wait()
        S2[...] = S1[keep, :] + s1r[k % 2, keep, :].astype(F32)

    def after_y(k):
        y_copy(k).wait()
        S3[...] = S2[...] + s2r[k % 2].astype(F32)
        s3s[...] = S3[...].astype(BF)
        for copy in z_copies(k):
            copy.start()

    def after_z(k):
        for copy in z_copies(k):
            copy.wait()
        total = S3[:, lanes(z)]
        for j in range(3):
            total += s3r[k % 2, j].astype(F32)
        piece(k)[...] = total.astype(BF)
        for copy in (*out_z(k), out_y(k)[0]):
            copy.start()

    def hand_on(k):
        for copy in out_z(k):
            copy.wait_recv()
        for copy in out_y(k)[1:]:
            copy.start()

    def after_all(k):
        for copy in out_z(k):
            copy.wait_send()
        for copy in out_y(k):
            copy.wait()
        layer, c = 1 - k // CHUNKS, k % CHUNKS
        for q in range(2):
            for n, (out, half) in enumerate(((og_ref, 0), (og_ref, CHUNKS), (ou_ref, 0), (ou_ref, CHUNKS))):
                src = fin.at[k, 96 * q : 96 * q + 64, 128 * n : 128 * n + 128]
                dst = out.at[layer, 64 * q : 64 * q + 64, lanes(c + half)]
                pltpu.make_async_copy(src, dst, osem.at[layer, n // 2]).start()

    def when(cond, f, k):
        pl.when(cond)(lambda: f(k))

    def into(layer, t, n):
        at = pl.ds(pl.multiple_of(t * n, n), n)
        by_a = nt(DGU[0, at, :], W[layer, 0])
        for c in range(1, CHUNKS):
            by_a += nt(DGU[c, at, :], W[layer, c])
        by_a = by_a.astype(BF).astype(F32)
        wide = XH[at, :].astype(F32)
        scale = scale_of(wide)
        back = by_a * scale - wide * (scale * scale * scale * jnp.mean(by_a * wide, -1, keepdims=True))
        G[at, :] = (G[at, :].astype(F32) + back.astype(BF).astype(F32)).astype(BF)

    load_a = pltpu.make_async_copy(dx_ref, A, asem.at[4])

    def step(k, carry):
        layer, c = 1 - k // CHUNKS, k % CHUNKS

        @pl.when(k == CHUNKS)
        def _():
            load_a.start()

            def one(t, carry):
                into(1, t, tt)
                return carry

            lax.fori_loop(0, 4, one, 0)
            for copy in load_x:
                copy.start()
            load_a.wait()

        @pl.when(k < CHUNKS)
        def _():
            @pl.when(k + 3 < CHUNKS)
            def _():
                pass_x(1, k + 3)

            @pl.when(k + 1 < CHUNKS)
            def _():
                pass_y(1, k + 1)

            arrived(1, k)

        rows = pl.ds(pl.multiple_of(256 * c, 256), 256)

        def front(t):
            gu = nn(A[tile[t], :], W[layer, c])
            gate, up = gu[:, 0:256], gu[:, 256:512]
            by_act = nt(G[tile[t], :], WD[layer, rows, :]).astype(BF).astype(F32)
            sig, silu = gated(gate)
            AC2[t % 2] = (silu * up).astype(BF)
            DGU[c, tile[t], 0:256] = (by_act * up * (sig * (1.0 + (gate - silu)))).astype(BF)
            DGU[c, tile[t], 256:512] = (by_act * silu).astype(BF)

        def back(t):
            gu, dn = tn(A[tile[t], :], DGU[c, tile[t], :]), tn(AC2[t % 2], G[tile[t], :])
            ACC[...] = ACC[...] + gu if t else gu
            ACD[...] = ACD[...] + dn if t else dn

        front(0)
        front(1)
        back(0)
        when(k >= 2, after_x, k - 2)
        when(k >= 1, after_core, k - 1)
        front(2)
        back(1)
        front(3)
        back(2)
        back(3)
        when(k >= 5, after_all, k - 5)
        when(k >= 4, hand_on, k - 4)
        when(k >= 3, after_z, k - 3)
        when(k >= 2, after_y, k - 2)
        send_core()
        core_copy(k).start()
        return carry

    lax.fori_loop(0, STEPS, step, 0)

    last = STEPS - 1
    e = tokens // 8
    eighth = [pl.ds(i * e, e) for i in range(8)]
    store_dx = [pltpu.make_async_copy(G.at[t, :], dx_ref.at[t, :], asem.at[i]) for i, t in enumerate(eighth)]

    def by_x(i):
        into(0, i, e)
        store_dx[i].start()

    def down_copies(layer):
        first = (1 - layer) * CHUNKS + (CHUNKS - 2) * (1 - core)
        return [
            remote(fin.at[pl.ds(first, 2), 96 * q + 64 : 96 * q + 96, :], dnx.at[layer, :, 32 * q : 32 * q + 32, :], dns.at[layer, q], dnr.at[layer, q], partner)
            for q in range(2)
        ]

    def put_down(layer):
        for copy in down_copies(layer):
            copy.wait()
        copies = []
        for n in range(3):
            for q in range(2):
                src = fin.at[(1 - layer) * CHUNKS + n + 2 * core, 96 * q + 64 : 96 * q + 96, :]
                copies.append((src, od_ref.at[layer, 128 * n + 32 * q : 128 * n + 32 * q + 32, :]))
        for n in range(2):
            copies.append((dnx.at[layer, n], od_ref.at[layer, 128 * n + 64 : 128 * n + 128, :]))
        for src, dst in copies:
            pltpu.make_async_copy(src, dst, osem.at[layer, 2]).start()

    for copy in load_x:
        copy.wait()
    for copy in down_copies(1):
        copy.start()
    after_x(last - 1)
    by_x(0)
    after_core(last)
    after_z(last - 2)
    hand_on(last - 3)
    by_x(1)
    after_y(last - 1)
    after_all(last - 4)
    by_x(2)
    by_x(3)
    hand_on(last - 2)
    after_all(last - 3)
    after_x(last)
    by_x(4)
    after_z(last - 1)
    by_x(5)
    after_y(last)
    put_down(1)
    by_x(6)
    hand_on(last - 1)
    after_all(last - 2)
    by_x(7)
    after_z(last)
    after_all(last - 1)
    for layer in range(2):
        for row in range(5):
            for p in range(CHUNKS + 5):
                fetch(layer, p, KINDS[row]).wait_send()
    hand_on(last)
    after_all(last)
    for copy in down_copies(0):
        copy.start()
    put_down(0)
    for copy in store_dx:
        copy.wait()
    for layer in range(2):
        for n, out in enumerate((og_ref, ou_ref, od_ref)):
            pltpu.make_async_copy(out.at[layer], out.at[layer], osem.at[layer, n]).wait()


def place_results(*refs):
    sources, results, held, (rsem, wsem) = refs[:4], refs[4:8], refs[8:12], refs[12:]
    n = sources[0].shape[0] // 8
    cuts = [(0, pl.ds(i * n, n)) for i in range(8)] + [(j, layer) for j in range(1, 4) for layer in range(LAYERS)]
    reads = [pltpu.make_async_copy(sources[j].at[at], held[j].at[at], rsem.at[i]) for i, (j, at) in enumerate(cuts)]
    writes = [pltpu.make_async_copy(held[j].at[at], results[j].at[at], wsem.at[i]) for i, (j, at) in enumerate(cuts)]
    for copy in reads:
        copy.start()
    for read, write in zip(reads, writes, strict=True):
        read.wait()
        write.start()
    for copy in writes:
        copy.wait()


def solution(mesh):
    def step(x, dy, wg, wu, wd):
        tokens = x.shape[1]
        tt = tokens // 4
        hbm = pl.BlockSpec(memory_space=pl.ANY)
        V, DMA = pltpu.VMEM, pltpu.SemaphoreType.DMA
        dx, *grads = pl.pallas_call(
            kernel,
            out_shape=[
                jax.ShapeDtypeStruct((tokens, D), BF),
                *(jax.ShapeDtypeStruct(w.shape, BF) for w in (wg, wu, wd)),
            ],
            in_specs=[hbm] * 5,
            out_specs=[hbm] * 4,
            scratch_shapes=[
                V((LAYERS, CHUNKS, D, 512), BF), V((LAYERS, FF, D), BF),
                V((tokens, D), BF), V((tokens, D), BF), V((tokens, D), BF), V((CHUNKS, tokens, 512), BF),
                V((D, 512), F32), V((256, D), F32), V((2, tt, 256), BF),
                V((2, 192, 512), F32), V((2, 192, 512), BF), V((2, 2, 192, 512), BF),
                V((192, 512), F32), V((192, 512), BF), V((2, 192, 512), BF),
                V((96, 512), F32), V((96, 512), BF), V((2, 96, 512), BF),
                V((96, 512), F32), V((96, 512), BF), V((2, 3, 96, 128), BF),
                V((STEPS, 192, 512), BF), V((LAYERS, 2, 64, 512), BF),
                DMA((LAYERS, CHUNKS, 4)), DMA((LAYERS, 5)), DMA((5,)), DMA((8,)), DMA((LAYERS, 3)),
                DMA((LAYERS, 5, CHUNKS + 5)), DMA((LAYERS, 5, CHUNKS + 5)), DMA((4, 2)), DMA((4, 2)),
                DMA((2, 3)), DMA((2, 3)), DMA((4, 3)), DMA((4, 3)), DMA((4, 4)), DMA((4, 4)), DMA((2, 2)), DMA((2, 2)),
            ],
            compiler_params=pltpu.CompilerParams(collective_id=0, has_side_effects=True, vmem_limit_bytes=67_043_328),
        )(x[0], dy[0], wg, wu, wd)
        V, DMA = pltpu.VMEM, pltpu.SemaphoreType.DMA
        results = (dx, *grads)
        dx, *grads = pl.pallas_call(
            place_results,
            out_shape=[jax.ShapeDtypeStruct(a.shape, BF) for a in results],
            in_specs=[hbm] * 4,
            out_specs=[hbm] * 4,
            scratch_shapes=[*(V(a.shape, BF) for a in results), DMA((14,)), DMA((14,))],
            compiler_params=pltpu.CompilerParams(vmem_limit_bytes=60_000_000),
        )(*results)
        return (dx[None], *grads)

    states, cut = P(("rep", "r", "s"), None, None), P(None, "s", None)
    return jax.shard_map(
        step,
        mesh=mesh,
        in_specs=(states, states) + (cut,) * 3,
        out_specs=(states,) + (P("rep", "s", None),) * 3,
        check_vma=False,
    )
```

```python
import functools

import jax
import jax.numpy as jnp
from jax import lax
from jax.experimental import pallas as pl
from jax.experimental.pallas import tpu as pltpu
from jax.sharding import PartitionSpec as P

MESH = pl.DeviceIdType.MESH
BF, F32 = jnp.bfloat16, jnp.float32
LAYERS, D, FF = 2, 512, 1280
HALF = FF // 2
CHUNKS = HALF // 128
STEPS = LAYERS * CHUNKS


def nn(a, b):
    return jnp.dot(a, b, preferred_element_type=F32)


def nt(a, b):
    return lax.dot_general(a, b, (((1,), (1,)), ((), ())), preferred_element_type=F32)


def tn(a, b):
    return lax.dot_general(a, b, (((0,), (0,)), ((), ())), preferred_element_type=F32)


def scale_of(wide):
    return lax.rsqrt(jnp.mean(wide * wide, -1, keepdims=True) + 1e-6)


def gated(gate):
    sig = 0.5 * jnp.tanh(0.5 * gate) + 0.5
    return sig, gate * sig


def kernel(
    x_ref, dy_ref, wg_ref, wu_ref, wd_ref,
    G, og_ref, ou_ref, od_ref, a_ref,
    W, WD, XH, A, DGU, ACC, ACD, AC2,
    S0, s0s, s0r, S1, s1s, s1r, S2, s2s, s2r, S3, s3s, s3r, near8, fin, dnx,
    lsem, ldsem, xsem, asem, gss, grs, ss, rs, zs, zr, azs, azr, ays, ayr, dns, dnr, n8s, n8r, a8s, a8r,
):
    r, s = lax.axis_index("r"), lax.axis_index("s")
    y, z = r // 4, r % 4
    xx, core = s // 2, s % 2
    tokens = XH.shape[0]
    tt = tokens // 4
    partner = {"s": 2 * xx + (1 - core)}
    xn = {"s": 2 * (1 - xx) + core}

    def place(dy_, dz_):
        return {"r": ((y + dy_) % 2) * 4 + (z + dz_) % 4}

    others = [(a, b) for a in range(2) for b in range(4) if (a, b) != (0, 0)]

    def lanes(n):
        return pl.ds(pl.multiple_of(128 * n, 128), 128)

    def some(start, n):
        return pl.ds(pl.multiple_of(start, 32), n)

    def remote(src, dst, send, recv, dev):
        return pltpu.make_async_remote_copy(src_ref=src, dst_ref=dst, send_sem=send, recv_sem=recv, device_id=dev, device_id_type=MESH)

    def local_gu(layer, c, n):
        shard, half = ((wg_ref, 0), (wg_ref, CHUNKS), (wu_ref, 0), (wu_ref, CHUNKS))[n]
        return pltpu.make_async_copy(shard.at[layer, :, lanes(c + half)], W.at[layer, c, some(128 * s, 128), 128 * n : 128 * n + 128], lsem.at[layer, c, n])

    def unit(who, layer, i):
        n = 5 * (who % 2) + i
        return 256 * (n // 2) + 128 * (who // 2) + 64 * (n % 2)

    def local_d(layer, i):
        return pltpu.make_async_copy(wd_ref.at[layer, 64 * i : 64 * i + 64, :], WD.at[layer, some(unit(s, layer, i), 64), :], ldsem.at[layer, i])

    tile = [pl.ds(t * tt, tt) for t in range(4)]
    load_x = [pltpu.make_async_copy(x_ref.at[t, :], XH.at[t, :], xsem.at[i]) for i, t in enumerate(tile)]
    load_dy = pltpu.make_async_copy(dy_ref, G, xsem.at[4])
    for c in range(CHUNKS):
        for n in range(4):
            local_gu(0, c, n).start()
    for copy in load_x:
        copy.start()
    for i in range(5):
        local_d(0, i).start()
    for c in range(CHUNKS):
        for n in range(4):
            local_gu(1, c, n).start()
    for i in range(5):
        local_d(1, i).start()
    load_dy.start()

    barrier = pltpu.get_barrier_semaphore()
    for dev in [partner, xn] + [place(*o) for o in others]:
        pl.semaphore_signal(barrier, inc=1, device_id=dev, device_id_type=MESH)
    pl.semaphore_wait(barrier, 2 + len(others))

    far = 2 * (1 - xx) + core
    KINDS = ("near", "across", "to_y", "mine_near", "other_near")

    def fetch(layer, p, kind):
        who = s if kind in ("near", "across") else far
        row = KINDS.index(kind)
        dev = (partner, xn, place(1, 0), partner, partner)[row]
        half = 1 - y if kind == "other_near" else y
        if isinstance(p, int) and p >= CHUNKS:
            start = unit(who, layer, p - CHUNKS)
            ref = WD.at[layer, some(start, 64) if kind == "near" else some(start + 32 * half, 32), :]
        else:
            ref = W.at[layer, p, some(128 * who, 128) if kind == "near" else some(128 * who + 64 * half, 64), :]
        return remote(ref, ref, gss.at[layer, row, p], grs.at[layer, row, p], dev)

    def begin(layer, p):
        if p >= CHUNKS:
            local_d(layer, p - CHUNKS).wait()
        else:
            for n in range(4):
                local_gu(layer, p, n).wait()
        fetch(layer, p, "across").start()
        fetch(layer, p, "near").start()

    def pass_x(layer, p):
        fetch(layer, p, "across").wait_recv()
        fetch(layer, p, "to_y").start()
        fetch(layer, p, "mine_near").start()

    def pass_y(layer, p):
        fetch(layer, p, "to_y").wait_recv()
        fetch(layer, p, "other_near").start()

    def arrived(layer, p):
        for kind in ("near", "mine_near", "other_near"):
            fetch(layer, p, kind).wait_recv()

    downs = range(CHUNKS, CHUNKS + 5)
    for p in range(CHUNKS + 5):
        begin(0, p)
    save_a = [pltpu.make_async_copy(A.at[t, :], a_ref.at[t, :], asem.at[i]) for i, t in enumerate(tile)]
    for t in range(4):
        load_x[t].wait()
        wide = XH[tile[t], :].astype(F32)
        A[tile[t], :] = (wide * scale_of(wide)).astype(BF)
        save_a[t].start()

    pass_x(0, 0)
    pass_x(0, 1)
    pass_x(0, 2)
    pass_y(0, 0)

    def up_front(c, carry):
        @pl.when(c + 3 < CHUNKS)
        def _():
            pass_x(0, c + 3)

        @pl.when(c + 1 < CHUNKS)
        def _():
            pass_y(0, c + 1)

        @pl.when(c == 3)
        def _():
            for p in downs:
                pass_x(0, p)
            for p in downs:
                begin(1, p)

        @pl.when(c == 4)
        def _():
            for p in downs:
                pass_y(0, p)
            for p in range(CHUNKS):
                begin(1, p)

        arrived(0, c)
        for t in range(4):
            gu = nn(A[tile[t], :], W[0, c])
            gate, up = gu[:, 0:256], gu[:, 256:512]
            DGU[c // 2, tile[t], pl.ds(pl.multiple_of(256 * (c % 2), 256), 256)] = (gated(gate)[1] * up).astype(BF)
        return carry

    lax.fori_loop(0, CHUNKS, up_front, 0)
    for p in downs:
        arrived(0, p)
    for copy in save_a:
        copy.wait()

    def down_back(t):
        out = nn(DGU[0, tile[t], :], WD[0, 0:512, :]) + nn(DGU[1, tile[t], :], WD[0, 512:1024, :]) + nn(DGU[2, tile[t], 0:256], WD[0, 1024:1280, :])
        h = (XH[tile[t], :].astype(F32) + out.astype(BF).astype(F32)).astype(BF)
        XH[tile[t], :] = h
        wide = h.astype(F32)
        A[tile[t], :] = (wide * scale_of(wide)).astype(BF)

    down_back(0)
    down_back(1)
    down_back(2)
    for p in downs:
        pass_x(1, p)
    down_back(3)
    for p in range(3):
        pass_x(1, p)
    for p in downs:
        pass_y(1, p)
    pass_y(1, 0)
    for p in downs:
        arrived(1, p)
    load_dy.wait()

    def pair(k, j, dev, src, dst):
        return remote(src, dst, ss.at[j, k % 2], rs.at[j, k % 2], dev)

    def core_copy(k):
        return pair(k, 0, partner, s0s, s0r.at[k % 2])

    def x_copies(k):
        return [pair(k, 1 + i, xn, s1s.at[some(96 * h, 96), :], s1r.at[k % 2, some(96 * h, 96), :]) for i, h in enumerate((1 - y, y))]

    def y_copy(k):
        return pair(k, 3, place(1, 0), s2s, s2r.at[k % 2])

    def z_copies(k):
        return [
            remote(s3s.at[k % 2, :, lanes((z + j) % 4)], s3r.at[k % 2, j - 1], zs.at[k % 2, j - 1], zr.at[k % 2, j - 1], place(0, j)) for j in range(1, 4)
        ]

    def piece(k, z_=z):
        return fin.at[k, some(96 * y, 96), lanes(z_)]

    def out_z(k):
        return [remote(piece(k), piece(k), azs.at[k % 4, j - 1], azr.at[k % 4, j - 1], place(0, j)) for j in range(1, 4)]

    def out_y(k):
        return [remote(piece(k, (z + j) % 4), piece(k, (z + j) % 4), ays.at[k % 4, j], ayr.at[k % 4, j], place(1, 0)) for j in range(4)]

    def send_core():
        for x_ in range(2):
            for q in range(2):
                for buf, who in ((s0s, 1 - core), (S0, core)):
                    gu = ACC[pl.ds(pl.multiple_of(256 * x_ + 128 * who + 64 * q, 64), 64), :]
                    dn = ACD[some(128 * x_ + 64 * who + 32 * q, 32), :]
                    buf[x_, 96 * q : 96 * q + 64, :] = gu.astype(buf.dtype)
                    buf[x_, 96 * q + 64 : 96 * q + 96, :] = dn.astype(buf.dtype)

    def after_core(k):
        core_copy(k).wait()
        for copy, h in zip(x_copies(k), (1 - y, y), strict=True):
            half = some(96 * h, 96)
            s1s[half, :] = (S0[1 - xx, half, :] + s0r[k % 2, 1 - xx, half, :].astype(F32)).astype(BF)
            copy.start()
        S1[...] = S0[xx] + s0r[k % 2, xx].astype(F32)

    def after_x(k):
        x_copies(k)[0].wait()
        give, keep = (some(96 * h, 96) for h in (1 - y, y))
        s2s[...] = (S1[give, :] + s1r[k % 2, give, :].astype(F32)).astype(BF)
        y_copy(k).start()
        x_copies(k)[1].wait()
        S2[...] = S1[keep, :] + s1r[k % 2, keep, :].astype(F32)

    def after_y(k):
        y_copy(k).wait()
        S2[...] += s2r[k % 2].astype(F32)
        s3s[k % 2] = S2[...].astype(BF)
        for copy in z_copies(k):
            copy.start()
        S3[k % 2] = S2[:, lanes(z)]

    def after_z(k):
        for copy in z_copies(k):
            copy.wait()
        send_out(k, [s3r[k % 2, j] for j in range(3)], lambda k: (*out_z(k), out_y(k)[0]))

    def send_out(k, terms, copies):
        total = S3[k % 2]
        for term in terms:
            total += term.astype(F32)
        piece(k)[...] = total.astype(BF)
        for copy in copies(k):
            copy.start()

    def out_all(k):
        return [remote(piece(k), piece(k), a8s.at[i], a8r.at[i], place(*o)) for i, o in enumerate(others)]

    def to_all(src, dy_, dzs):
        return [remote(src.at[:, lanes((z + j) % 4)], near8.at[4 * dy_ + j - 1], n8s.at[4 * dy_ + j - 1], n8r.at[4 * dy_ + j - 1], place(dy_, j)) for j in dzs]

    def last_over_y(k):
        x_copies(k)[0].wait()
        give = some(96 * (1 - y), 96)
        s2s[...] = (S1[give, :] + s1r[k % 2, give, :].astype(F32)).astype(BF)
        for copy in to_all(s2s, 1, range(4)):
            copy.start()

    def last_over_z(k):
        x_copies(k)[1].wait()
        keep = some(96 * y, 96)
        S2[...] = S1[keep, :] + s1r[k % 2, keep, :].astype(F32)
        s3s[k % 2] = S2[...].astype(BF)
        for copy in to_all(s3s.at[k % 2], 0, range(1, 4)):
            copy.start()
        S3[k % 2] = S2[:, lanes(z)]

    def last_sum(k):
        for copy in (*to_all(s2s, 1, range(4)), *to_all(s3s.at[k % 2], 0, range(1, 4))):
            copy.wait()
        send_out(k, [near8[j] for j in range(7)], out_all)

    def hand_on(k):
        for copy in out_z(k):
            copy.wait_recv()
        for copy in out_y(k)[1:]:
            copy.start()

    def after_all(k):
        for copy in out_z(k):
            copy.wait_send()
        for copy in out_y(k):
            copy.wait()
        put_chunk(k)

    def put_chunk(k):
        layer, c = 1 - k // CHUNKS, k % CHUNKS
        for q in range(2):
            for n, (out, half) in enumerate(((og_ref, 0), (og_ref, CHUNKS), (ou_ref, 0), (ou_ref, CHUNKS))):
                out[layer, 64 * q : 64 * q + 64, lanes(c + half)] = fin[k, 96 * q : 96 * q + 64, 128 * n : 128 * n + 128]

    def when(cond, f, k):
        pl.when(cond)(lambda: f(k))

    def into(layer, t, n):
        at = pl.ds(pl.multiple_of(t * n, n), n)
        by_a = nt(DGU[0, at, :], W[layer, 0])
        for c in range(1, CHUNKS):
            by_a += nt(DGU[c, at, :], W[layer, c])
        by_a = by_a.astype(BF).astype(F32)
        wide = XH[at, :].astype(F32)
        scale = scale_of(wide)
        back = by_a * scale - wide * (scale * scale * scale * jnp.mean(by_a * wide, -1, keepdims=True))
        G[at, :] = (G[at, :].astype(F32) + back.astype(BF).astype(F32)).astype(BF)

    load_a = pltpu.make_async_copy(a_ref, A, asem.at[4])

    e = tokens // 8

    def step(k, carry):
        layer, c = 1 - k // CHUNKS, k % CHUNKS

        @pl.when(k == CHUNKS)
        def _():
            load_a.start()

            def one(t, carry):
                into(1, 2 * t, e)
                into(1, 2 * t + 1, e)
                return carry

            lax.fori_loop(0, 4, one, 0)
            for copy in load_x:
                copy.start()
            load_a.wait()

        @pl.when(k < CHUNKS)
        def _():
            @pl.when(k + 3 < CHUNKS)
            def _():
                pass_x(1, k + 3)

            @pl.when(k + 1 < CHUNKS)
            def _():
                pass_y(1, k + 1)

            arrived(1, k)

        rows = pl.ds(pl.multiple_of(256 * c, 256), 256)

        def front(t):
            gu = nn(A[tile[t], :], W[layer, c])
            gate, up = gu[:, 0:256], gu[:, 256:512]
            by_act = nt(G[tile[t], :], WD[layer, rows, :]).astype(BF).astype(F32)
            sig, silu = gated(gate)
            AC2[t % 2] = (silu * up).astype(BF)
            DGU[c, tile[t], 0:256] = (by_act * up * (sig * (1.0 + (gate - silu)))).astype(BF)
            DGU[c, tile[t], 256:512] = (by_act * silu).astype(BF)

        def back(t):
            gu, dn = tn(A[tile[t], :], DGU[c, tile[t], :]), tn(AC2[t % 2], G[tile[t], :])
            ACC[...] = ACC[...] + gu if t else gu
            ACD[...] = ACD[...] + dn if t else dn

        front(0)
        front(1)
        back(0)
        when(k >= 2, after_x, k - 2)
        when(k >= 1, after_core, k - 1)
        front(2)
        back(1)
        front(3)
        back(2)
        back(3)
        when(k >= 5, after_all, k - 5)
        when(k >= 4, hand_on, k - 4)
        when(k >= 3, after_z, k - 3)
        when(k >= 2, after_y, k - 2)
        send_core()
        core_copy(k).start()
        return carry

    lax.fori_loop(0, STEPS, step, 0)

    last = STEPS - 1
    def by_x(i):
        into(0, i, e)

    def down_copies(layer):
        first = (1 - layer) * CHUNKS + (CHUNKS - 2) * (1 - core)
        return [
            remote(fin.at[pl.ds(first, 2), 96 * q + 64 : 96 * q + 96, :], dnx.at[layer, :, 32 * q : 32 * q + 32, :], dns.at[layer, q], dnr.at[layer, q], partner)
            for q in range(2)
        ]

    def put_down(layer):
        for copy in down_copies(layer):
            copy.wait()
        for n in range(3):
            for q in range(2):
                block = fin[(1 - layer) * CHUNKS + n + 2 * core, 96 * q + 64 : 96 * q + 96, :]
                od_ref[layer, 128 * n + 32 * q : 128 * n + 32 * q + 32, :] = block
        for n in range(2):
            od_ref[layer, 128 * n + 64 : 128 * n + 128, :] = dnx[layer, n]

    for copy in load_x:
        copy.wait()
    for copy in down_copies(1):
        copy.start()
    by_x(0)
    after_x(last - 1)
    after_core(last)
    by_x(1)
    after_all(last - 4)
    hand_on(last - 3)
    by_x(2)
    after_z(last - 2)
    after_y(last - 1)
    last_over_y(last)
    by_x(3)
    last_over_z(last)
    by_x(4)
    hand_on(last - 2)
    after_all(last - 3)
    by_x(5)
    after_z(last - 1)
    by_x(6)
    last_sum(last)
    by_x(7)
    put_down(1)
    hand_on(last - 1)
    after_all(last - 2)
    for layer in range(2):
        for row in range(5):
            for p in range(CHUNKS + 5):
                fetch(layer, p, KINDS[row]).wait_send()
    after_all(last - 1)
    for copy in out_all(last):
        copy.wait()
    put_chunk(last)
    for copy in down_copies(0):
        copy.start()
    put_down(0)


def place_results(*refs):
    copies = [pltpu.make_async_copy(refs[i], refs[4 + i], refs[8].at[i]) for i in range(4)]
    for copy in copies:
        copy.start()
    for copy in copies:
        copy.wait()


def solution(mesh):
    def step(x, dy, wg, wu, wd):
        tokens = x.shape[1]
        tt = tokens // 4
        hbm, vmem = pl.BlockSpec(memory_space=pl.ANY), pl.BlockSpec(memory_space=pltpu.VMEM)
        V, DMA = pltpu.VMEM, pltpu.SemaphoreType.DMA
        dx, *grads, _ = pl.pallas_call(
            kernel,
            out_shape=[
                V((tokens, D), BF),
                *(V(w.shape, BF) for w in (wg, wu, wd)),
                jax.ShapeDtypeStruct((tokens, D), BF),
            ],
            in_specs=[hbm] * 5,
            out_specs=[vmem] * 4 + [hbm],
            scratch_shapes=[
                V((LAYERS, CHUNKS, D, 512), BF), V((LAYERS, FF, D), BF),
                V((tokens, D), BF), V((tokens, D), BF), V((CHUNKS, tokens, 512), BF),
                V((D, 512), F32), V((256, D), F32), V((2, tt, 256), BF),
                V((2, 192, 512), F32), V((2, 192, 512), BF), V((2, 2, 192, 512), BF),
                V((192, 512), F32), V((192, 512), BF), V((2, 192, 512), BF),
                V((96, 512), F32), V((96, 512), BF), V((2, 96, 512), BF),
                V((2, 96, 128), F32), V((2, 96, 512), BF), V((2, 3, 96, 128), BF), V((7, 96, 128), BF),
                V((STEPS, 192, 512), BF), V((LAYERS, 2, 64, 512), BF),
                DMA((LAYERS, CHUNKS, 4)), DMA((LAYERS, 5)), DMA((5,)), DMA((5,)),
                DMA((LAYERS, 5, CHUNKS + 5)), DMA((LAYERS, 5, CHUNKS + 5)), DMA((4, 2)), DMA((4, 2)),
                DMA((2, 3)), DMA((2, 3)), DMA((4, 3)), DMA((4, 3)), DMA((4, 4)), DMA((4, 4)), DMA((2, 2)), DMA((2, 2)), DMA((7,)), DMA((7,)), DMA((7,)), DMA((7,)),
            ],
            compiler_params=pltpu.CompilerParams(collective_id=0, has_side_effects=True, vmem_limit_bytes=60_500_000),
        )(x[0], dy[0], wg, wu, wd)
        V, DMA = pltpu.VMEM, pltpu.SemaphoreType.DMA
        results = (dx, *grads)
        dx, *grads = pl.pallas_call(
            place_results,
            out_shape=[jax.ShapeDtypeStruct(a.shape, BF) for a in results],
            in_specs=[vmem] * 4,
            out_specs=[hbm] * 4,
            scratch_shapes=[DMA((4,))],
            compiler_params=pltpu.CompilerParams(vmem_limit_bytes=16_000_000),
        )(*results)
        return (dx[None], *grads)

    states, cut = P(("rep", "r", "s"), None, None), P(None, "s", None)
    return jax.shard_map(
        step,
        mesh=mesh,
        in_specs=(states, states) + (cut,) * 3,
        out_specs=(states,) + (P("rep", "s", None),) * 3,
        check_vma=False,
    )
```
